32 devices in a mesh: row: 4 (over y, x), col: 8 (over z, core).
Axes of the slice: x: 2, y: 2, z: 4, core: 2. Of those that a mesh axis runs over, the one named last changes fastest.
Arguments:
- h_old: float32 [4, 8, 2048, 4096], P('row', 'col'), may hold values from -2 to 2, as said below
- s_old: float32 [4, 8, 2048, 128], P('row', 'col'), may hold values from -100 to 100, as said below
- row_owner: int32 [256], replicated, may hold values from 0 to 7, as said below
- col_owner: int32 [256], replicated, may hold values from 0 to 3, as said below
Outputs:
- h_reduced: float32 [16384, 16384], P('row', 'col')
- panel_factor: float32 [16384, 512], P('row')
The draws below stay inside these ranges and needn't reach their ends.
Inputs may be any that keep to these rules, and one draw needn't show every extreme that they name: `row_owner`: each aligned run of 8 entries is an ordering of 0 to 7. `col_owner`: each aligned run of 4 entries is an ordering of 0 to 3. `s_old`: the first 512 rows of S_panel form a symmetric positive definite matrix. `h_old`: H is symmetric.
All inputs are finite; a program needn't handle non-finite values.
Results may differ from the reference program's by a relative error of at most 0.00017.
Values sent between devices are 32-bit elements; how exact they have to be, the bound alone decides.
A program may use at most 320 MiB of HBM per device.

```python
from functools import partial
import jax
import jax.numpy as jnp
from jax import lax

ORDER = 16384
PANEL = 512
BLOCK = 64
OLD_ROWS = 8
OLD_COLS = 4
N_ROW = 4
N_COL = 8


def shuffled(subkey, count):
    return jax.random.permutation(subkey, count)


def owner_maps(key):
    base = jax.random.fold_in(key, 7001)
    row_keys = jax.random.split(jax.random.fold_in(base, 1), ORDER // (BLOCK * OLD_ROWS))
    col_keys = jax.random.split(jax.random.fold_in(base, 2), ORDER // (BLOCK * OLD_COLS))
    rows = jax.vmap(partial(shuffled, count=OLD_ROWS))(row_keys).reshape(-1).astype(jnp.int32)
    cols = jax.vmap(partial(shuffled, count=OLD_COLS))(col_keys).reshape(-1).astype(jnp.int32)
    return (rows, cols)


def to_layout(natural, owner_rows, owner_cols):
    blocks_row = natural.shape[0] // BLOCK
    blocks_col = natural.shape[1] // BLOCK
    tiles = natural.reshape(blocks_row, BLOCK, blocks_col, BLOCK).transpose(0, 2, 1, 3)
    owner_row = owner_rows[:blocks_row][:, None]
    owner_col = owner_cols[:blocks_col][None, :]
    shape_two = (blocks_row, blocks_col)
    device_row = jnp.broadcast_to(owner_row // 2, shape_two)
    device_col = 2 * owner_col + owner_row % 2
    slot_row = jnp.broadcast_to((jnp.arange(blocks_row, dtype=jnp.int32) // OLD_ROWS)[:, None], shape_two)
    slot_col = jnp.broadcast_to((jnp.arange(blocks_col, dtype=jnp.int32) // OLD_COLS)[None, :], shape_two)
    stored = jnp.zeros((OLD_ROWS // 2, OLD_COLS * 2, blocks_row // OLD_ROWS, blocks_col // OLD_COLS, BLOCK, BLOCK), jnp.float32)
    stored = stored.at[device_row, device_col, slot_row, slot_col].set(tiles)
    return stored.transpose(0, 1, 2, 4, 3, 5).reshape(OLD_ROWS // 2, OLD_COLS * 2, blocks_row // OLD_ROWS * BLOCK, blocks_col // OLD_COLS * BLOCK)


def draw_row_owner(key, part):
    return owner_maps(key)[0]


def draw_col_owner(key, part):
    return owner_maps(key)[1]


def draw_h_old(key, part):
    owner_rows, owner_cols = owner_maps(key)
    subkey = jax.random.fold_in(key, 11)
    noise = jax.random.truncated_normal(subkey, -6.0, 6.0, (ORDER, ORDER), jnp.float32)
    natural = (noise + noise.T) * 0.15
    return to_layout(natural, owner_rows, owner_cols)


def draw_s_old(key, part):
    owner_rows, owner_cols = owner_maps(key)
    square = jax.random.truncated_normal(jax.random.fold_in(key, 21), -6.0, 6.0, (PANEL, PANEL), jnp.float32)
    diagonal = jax.random.uniform(jax.random.fold_in(key, 22), (PANEL,), jnp.float32, 3.0, 5.0)
    corner = (square + square.T) / jnp.sqrt(2.0 * PANEL) + jnp.diag(diagonal)
    below = 0.5 * jax.random.truncated_normal(jax.random.fold_in(key, 23), -6.0, 6.0, (ORDER - PANEL, PANEL), jnp.float32)
    natural = jnp.concatenate([corner, below], 0)
    return to_layout(natural, owner_rows, owner_cols)


def setup_inputs(seed: int = 0) -> dict:
    key_of = jax.random.split(jax.random.key(seed), 5)
    h_old = draw_h_old(jax.random.fold_in(key_of[4], 71), 0)
    s_old = draw_s_old(jax.random.fold_in(key_of[4], 71), 0)
    row_owner = draw_row_owner(jax.random.fold_in(key_of[4], 71), 0)
    col_owner = draw_col_owner(jax.random.fold_in(key_of[4], 71), 0)
    return dict(h_old=h_old, s_old=s_old, row_owner=row_owner, col_owner=col_owner)


def from_layout(stored, owner_rows, owner_cols, blocks_col):
    blocks_row = owner_rows.shape[0]
    grid = stored.reshape(N_ROW, N_COL, stored.shape[2] // BLOCK, BLOCK, stored.shape[3] // BLOCK, BLOCK)
    owner_row = owner_rows[:, None]
    owner_col = owner_cols[:blocks_col][None, :]
    shape_two = (blocks_row, blocks_col)
    device_row = jnp.broadcast_to(owner_row // 2, shape_two)
    device_col = 2 * owner_col + owner_row % 2
    slot_row = jnp.broadcast_to((jnp.arange(blocks_row, dtype=jnp.int32) // OLD_ROWS)[:, None], shape_two)
    slot_col = jnp.broadcast_to((jnp.arange(blocks_col, dtype=jnp.int32) // OLD_COLS)[None, :], shape_two)
    picked = grid[device_row, device_col, slot_row, :, slot_col, :]
    return picked.transpose(0, 2, 1, 3).reshape(blocks_row * BLOCK, blocks_col * BLOCK)

def reference(h_old, s_old, row_owner, col_owner):
    h_full = from_layout(h_old, row_owner, col_owner, ORDER // BLOCK)
    s_panel = from_layout(s_old, row_owner, col_owner, PANEL // BLOCK)
    lower_factor = jnp.linalg.cholesky(s_panel[:PANEL])
    solved = lax.linalg.triangular_solve(lower_factor, s_panel.T, left_side=True, lower=True)
    panel_factor = solved.T
    coupling = lax.linalg.triangular_solve(lower_factor, solved, left_side=True, lower=True, transpose_a=True).T
    identity = jnp.eye(PANEL, dtype=jnp.float32)
    inverse = lax.linalg.triangular_solve(lower_factor, identity, left_side=True, lower=True)
    coupling = coupling.at[:PANEL].set(identity - inverse)
    h_panel = h_full[:, :PANEL]
    mixed = h_panel - 0.5 * jnp.dot(coupling, h_panel[:PANEL], precision=lax.Precision.HIGHEST)
    left_terms = jnp.concatenate([coupling, mixed], 1)
    right_terms = jnp.concatenate([mixed, coupling], 1)
    update = jnp.dot(left_terms, right_terms.T, precision=lax.Precision.HIGHEST)
    return (h_full - update, panel_factor)
```

```python
import functools

import jax
import jax.numpy as jnp
from jax import lax
from jax.experimental import pallas as pl
from jax.experimental.pallas import tpu as pltpu
from jax.sharding import PartitionSpec as P

ORDER = 16384
PANEL = 512
BLOCK = 64
HIGHEST = lax.Precision.HIGHEST


def pack_kernel(in_ref, out_ref):
    out_ref[0] = in_ref[...]


def pack(local, row_count, col_count):
    rows, cols = local.shape
    part_rows, part_cols = rows // row_count, cols // col_count
    return pl.pallas_call(
        pack_kernel,
        grid=(row_count, col_count),
        in_specs=[pl.BlockSpec((part_rows, part_cols), lambda i, j: (i, j))],
        out_specs=pl.BlockSpec(
            (1, part_rows, part_cols), lambda i, j: (i * col_count + j, 0, 0)
        ),
        out_shape=jax.ShapeDtypeStruct((row_count * col_count, part_rows, part_cols), local.dtype),
        cost_estimate=pl.CostEstimate(
            flops=0, bytes_accessed=2 * local.size * 4, transcendentals=0
        ),
        name="pack",
    )(local)


def panel_kernel(old_rows, old_cols, panel_local, panel_blocks, dev_row, dev_col, in_ref, s_ref, h_ref):
    group = pl.program_id(0)
    for gi in range(old_rows):
        row_part = dev_row[group * old_rows + gi]
        rows = pl.ds(gi * BLOCK, BLOCK)
        for base, out_ref in ((0, s_ref), (panel_local, h_ref)):
            for k in range(0, panel_blocks, 2):
                pair = []
                for kk in (k, k + 1):
                    start = base + kk // old_cols * BLOCK
                    pair.append(in_ref[row_part + dev_col[kk], :, start : start + BLOCK])
                out_ref[rows, k * BLOCK : (k + 2) * BLOCK] = jnp.concatenate(pair, axis=1)


def arrange_panel(gathered, dev_row, dev_col, old_rows, old_cols, panel_local):
    devices, part_rows, width = gathered.shape
    groups = part_rows // BLOCK
    height = old_rows * BLOCK
    shape = jax.ShapeDtypeStruct((groups * height, PANEL), jnp.float32)
    out_spec = pl.BlockSpec((height, PANEL), lambda g, *_: (g, 0))
    return pl.pallas_call(
        functools.partial(panel_kernel, old_rows, old_cols, panel_local, PANEL // BLOCK),
        grid_spec=pltpu.PrefetchScalarGridSpec(
            num_scalar_prefetch=2,
            grid=(groups,),
            in_specs=[pl.BlockSpec((devices, BLOCK, width), lambda g, *_: (0, g, 0))],
            out_specs=[out_spec, out_spec],
        ),
        out_shape=[shape, shape],
        cost_estimate=pl.CostEstimate(
            flops=0, bytes_accessed=2 * gathered.size * 4, transcendentals=0
        ),
        name="arrange_panel",
    )(dev_row, dev_col, gathered)


def split(x):
    high = x.astype(jnp.bfloat16)
    return high, (x - high.astype(jnp.float32)).astype(jnp.bfloat16)


def update_kernel(
    old_rows,
    old_cols,
    rounds_col,
    dev_row,
    dev_col,
    in_ref,
    left_n,
    left_q,
    right_q,
    right_n,
    out_ref,
    left_hi,
    left_lo,
    right_hi,
    right_lo,
):
    group = pl.program_id(0)

    @pl.when(group == 0)
    def _():
        right_hi[:, :PANEL], right_lo[:, :PANEL] = split(right_q[...])
        right_hi[:, PANEL:], right_lo[:, PANEL:] = split(right_n[...])

    left_hi[:, :PANEL], left_lo[:, :PANEL] = split(left_n[...])
    left_hi[:, PANEL:], left_lo[:, PANEL:] = split(left_q[...])
    span = 2 * old_cols * BLOCK

    def chunk(t, carry):
        cols = pl.ds(pl.multiple_of(t * span, span), span)
        dims = (((1,), (1,)), ((), ()))

        def product(a, b):
            return lax.dot_general(
                a[...], b[cols, :], dims, preferred_element_type=jnp.float32
            )

        update = (
            product(left_hi, right_lo) + product(left_lo, right_hi)
        ) + product(left_hi, right_hi)
        lanes = pl.ds(pl.multiple_of(t * 2 * BLOCK, 2 * BLOCK), 2 * BLOCK)
        for gi in range(old_rows):
            row_part = dev_row[group * old_rows + gi]
            top = gi * BLOCK
            for k in range(0, 2 * old_cols, 2):
                start = k // old_cols * BLOCK
                pair = []
                for kk in (k, k + 1):
                    device = row_part + dev_col[t * 2 * old_cols + kk]
                    pair.append(in_ref[device, :, lanes][:, start : start + BLOCK])
                block = jnp.concatenate(pair, axis=1)
                where = pl.ds(
                    pl.multiple_of(t * span + k * BLOCK, 2 * BLOCK), 2 * BLOCK
                )
                out_ref[top : top + BLOCK, where] = (
                    block - update[top : top + BLOCK, k * BLOCK : (k + 2) * BLOCK]
                )
        return carry

    lax.fori_loop(0, rounds_col // 2, chunk, 0)


def assemble_and_update(received, coupling, mixed, column_q, column_n, dev_row, dev_col, old_rows, old_cols):
    devices, part_rows, part_cols = received.shape
    groups = part_rows // BLOCK
    height = old_rows * BLOCK
    band = groups * height
    strip = column_q.shape[0]
    left_spec = pl.BlockSpec((height, PANEL), lambda g, *_: (g, 0))
    right_spec = pl.BlockSpec(
        (strip, PANEL), lambda g, *_: (0, 0), pipeline_mode=pl.Buffered(1)
    )
    return pl.pallas_call(
        functools.partial(update_kernel, old_rows, old_cols, part_cols // BLOCK),
        grid_spec=pltpu.PrefetchScalarGridSpec(
            num_scalar_prefetch=2,
            grid=(groups,),
            in_specs=[
                pl.BlockSpec((devices, BLOCK, part_cols), lambda g, *_: (0, g, 0)),
                left_spec,
                left_spec,
                right_spec,
                right_spec,
            ],
            out_specs=pl.BlockSpec((height, strip), lambda g, *_: (g, 0)),
            scratch_shapes=[
                pltpu.VMEM((height, 2 * PANEL), jnp.bfloat16),
                pltpu.VMEM((height, 2 * PANEL), jnp.bfloat16),
                pltpu.VMEM((strip, 2 * PANEL), jnp.bfloat16),
                pltpu.VMEM((strip, 2 * PANEL), jnp.bfloat16),
            ],
        ),
        out_shape=jax.ShapeDtypeStruct((band, strip), jnp.float32),
        cost_estimate=pl.CostEstimate(
            flops=3 * 4 * band * strip * PANEL,
            bytes_accessed=2 * received.size * 4,
            transcendentals=0,
        ),
        name="assemble_and_update",
    )(dev_row, dev_col, received, coupling, mixed, column_q, column_n)


def broadcast(block, axis, holder):
    block = jnp.where(lax.axis_index(axis) == holder, block, jnp.zeros_like(block))
    return lax.psum(block, axis)


def per_device(h_old, s_old, row_owner, col_owner):
    row_count = lax.axis_size("row")
    col_count = lax.axis_size("col")
    old_rows = 2 * row_count
    old_cols = col_count // 2
    row_id = lax.axis_index("row")
    col_id = lax.axis_index("col")
    local_h = h_old[0, 0]
    local_s = s_old[0, 0]
    rows_here, cols_here = local_h.shape
    part_rows = rows_here // row_count
    part_cols = cols_here // col_count
    band = ORDER // row_count
    strip = ORDER // col_count
    panel_local = local_s.shape[1]
    span_row = part_rows // BLOCK * old_rows
    span_col = part_cols // BLOCK * old_cols
    panel_blocks = PANEL // BLOCK
    owner_row = lax.dynamic_slice_in_dim(row_owner, row_id * span_row, span_row)
    owner_col = lax.dynamic_slice_in_dim(col_owner, col_id * span_col, span_col)

    panels = jnp.concatenate([local_s, local_h[:, :panel_local]], 1)
    corner_rows = -(-panel_blocks // old_rows) * BLOCK
    corners = lax.all_gather(panels[:corner_rows][None], ("row", "col"), axis=0, tiled=True)
    corner_owner = row_owner[: corner_rows // BLOCK * old_rows]
    panel_col = 2 * col_owner[:panel_blocks]
    corner_s, corner_h = arrange_panel(
        corners,
        corner_owner // 2 * col_count + corner_owner % 2,
        panel_col,
        old_rows,
        old_cols,
        panel_local,
    )
    corner_s, corner_h = corner_s[:PANEL], corner_h[:PANEL]

    pieces = panels.reshape(row_count, part_rows, 2 * panel_local)
    rows = lax.all_to_all(pieces, "row", split_axis=0, concat_axis=0, tiled=True)
    gathered = lax.all_gather(rows, "col", axis=0, tiled=True)
    s_panel, h_panel = arrange_panel(
        gathered,
        owner_row % 2 * row_count + owner_row // 2,
        panel_col * row_count,
        old_rows,
        old_cols,
        panel_local,
    )

    received = lax.all_to_all(
        pack(local_h, row_count, col_count),
        ("row", "col"),
        split_axis=0,
        concat_axis=0,
        tiled=True,
    )

    lower_factor = jnp.linalg.cholesky(corner_s)
    identity = jnp.eye(PANEL, dtype=jnp.float32)
    inverse = lax.linalg.triangular_solve(lower_factor, identity, left_side=True, lower=True)
    panel_factor = lax.dot_general(
        s_panel, inverse, (((1,), (1,)), ((), ())), precision=HIGHEST
    )
    coupling = jnp.dot(panel_factor, inverse, precision=HIGHEST)
    top_rows = jnp.concatenate(
        [identity - inverse, jnp.zeros((band - PANEL, PANEL), jnp.float32)], 0
    )
    leading = jnp.logical_and(row_id == 0, jnp.arange(band, dtype=jnp.int32)[:, None] < PANEL)
    coupling = jnp.where(leading, top_rows, coupling)
    mixed = h_panel - 0.5 * jnp.dot(coupling, corner_h, precision=HIGHEST)
    offset = col_id * strip % band
    root_row = col_id * strip // band
    column_n, column_q = (
        broadcast(lax.dynamic_slice_in_dim(coupling, offset, strip), "row", root_row),
        broadcast(lax.dynamic_slice_in_dim(mixed, offset, strip), "row", root_row),
    )
    h_reduced = assemble_and_update(
        received,
        coupling,
        mixed,
        column_q,
        column_n,
        owner_row // 2 * col_count + owner_row % 2,
        2 * owner_col,
        old_rows,
        old_cols,
    )
    return (h_reduced, panel_factor)


def solution(mesh):
    in_specs = (P("row", "col", None, None), P("row", "col", None, None), P(), P())
    out_specs = (P("row", "col"), P("row", None))
    return jax.shard_map(
        per_device, mesh=mesh, in_specs=in_specs, out_specs=out_specs, check_vma=False
    )
```
